32 devices in a mesh: section: 2 (over y), gx: 4 (over z), gy: 4 (over x, core).
Axes of the slice: x: 2, y: 2, z: 4, core: 2. Of those that a mesh axis runs over, the one named last changes fastest.
Arguments:
- fields: float32 [2, 4, 64, 256, 1024], P('section', None, None, 'gx', 'gy'), may hold values from -6 to 6
- slot_pick: int32 [4], replicated, may hold values from 0 to 3, each once
- courant_x: float32 [64, 256, 1024], P(None, 'gx', 'gy'), may hold values from 0.05 to 0.3
- courant_y: float32 [64, 256, 1024], P(None, 'gx', 'gy'), may hold values from 0.05 to 0.3
- horiz_diff: float32 [64], replicated, may hold values from 0.01 to 0.05
- vert_diff: float32 [64], replicated, may hold values from 0.01 to 0.1
- precip_class: int32 [256, 1024], P('gx', 'gy'), may hold values from 0 to 3
- class_rates: float32 [4], replicated, may hold values from 0.05 to 0.6
- vent_cells: int32 [64], replicated, may hold values from 0 to 262143
- vent_rate: float32 [64], replicated, may hold values from 0.5 to 2
- profile: float32 [64], replicated, may hold values from 0.05 to 1
Outputs:
- window_fields: float32 [2, 64, 256, 1024], P('section', None, 'gx', 'gy')
- sensitivity: float32 [64], replicated
The draws below stay inside these ranges and needn't reach their ends.
Inputs may be any that keep to these rules, and one draw needn't show every extreme that they name: `slot_pick`: each slot number appears once.
All inputs are finite; a program needn't handle non-finite values.
Results may differ from the reference program's by a relative error of at most 0.000088.
Values sent between devices are 32-bit elements; how exact they have to be, the bound alone decides.
No kernel may reach another device: no remote copies, remote signals or barrier semaphores. Data moves between devices by JAX's collectives and lax.ppermute only.
A program may use at most 192 MiB of HBM per device.

```python
import math
import jax
import jax.numpy as jnp

NZ = 64
SLOTS = 4
CLASSES = 4
VENTS = 64
NX = 256
NY = 1024


def touch_ends(entries, rng, smallest, high):
    longest = entries.shape.index(max(entries.shape))
    spots = []
    for shift in (0, 1):
        where = [jax.random.randint(jax.random.fold_in(rng, axis), (), 0, length) for axis, length in enumerate(entries.shape)]
        where[longest] = (where[longest] + shift) % entries.shape[longest]
        spots.append(tuple(where))
    return entries.at[spots[0]].set(smallest).at[spots[1]].set(high)


def level_of(own_key, shape, pieces, smallest, largest):
    gain = 1.0
    for dim, shards_of in pieces:
        draws = jax.random.uniform(jax.random.fold_in(jax.random.fold_in(own_key, 6), dim), (shards_of,), jnp.float32, smallest / len(pieces), largest / len(pieces))
        gain = gain * jnp.repeat(jnp.exp(draws), shape[dim] // shards_of).reshape((-1,) + (1,) * (len(shape) - 1 - dim))
    return gain


def scatter_about(key, shape, width, reach, cuts=(), held_as=jnp.bfloat16):
    factor_of = level_of(key, shape, cuts, -0.22, 0.18) if cuts else 1.0
    entries = jax.random.normal(key, shape, jnp.float32) * width * factor_of
    return jnp.minimum(jnp.maximum(entries, -reach), reach).astype(held_as)


def setup_inputs(seed: int = 0) -> dict:
    splits = jax.random.split(jax.random.key(seed), 12)
    return {
        "fields": scatter_about(splits[0], (2, SLOTS, NZ, NX, NY), 1.0, 6.0, ((0, 2), (3, 4), (4, 4)), jnp.float32),
        "slot_pick": jax.random.permutation(splits[1], SLOTS).astype(jnp.int32),
        "courant_x": jnp.clip(0.05 + 0.25 * jax.random.uniform(splits[2], (NZ, NX, NY), jnp.float32) ** level_of(splits[2], (NZ, NX, NY), ((1, 4), (2, 4)), -0.2, 0.2), 0.05, 0.3),
        "courant_y": jnp.clip(0.05 + 0.25 * jax.random.uniform(splits[3], (NZ, NX, NY), jnp.float32) ** level_of(splits[3], (NZ, NX, NY), ((1, 4), (2, 4)), -0.2, 0.2), 0.05, 0.3),
        "horiz_diff": jnp.clip(jnp.exp(jax.random.uniform(splits[4], (NZ,), jnp.float32, math.log(0.01), math.log(0.05))), 0.01, 0.05),
        "vert_diff": jnp.clip(jnp.exp(jax.random.uniform(splits[5], (NZ,), jnp.float32, math.log(0.01), math.log(0.1))), 0.01, 0.1),
        "precip_class": touch_ends(jax.random.randint(splits[6], (NX, NY), 0, CLASSES), jax.random.fold_in(splits[6], 1), 0, CLASSES - 1).astype(jnp.int32),
        "class_rates": jnp.clip(jnp.exp(jax.random.uniform(splits[7], (CLASSES,), jnp.float32, math.log(0.05), math.log(0.6))), 0.05, 0.6),
        "vent_cells": touch_ends(jax.random.randint(splits[8], (VENTS,), 0, NX * NY), jax.random.fold_in(splits[8], 1), 0, (NX * NY) - 1).astype(jnp.int32),
        "vent_rate": jnp.clip(jax.random.uniform(splits[9], (VENTS,), jnp.float32, 0.5, 2.0), 0.5, 2.0),
        "profile": jnp.clip(jnp.exp(jax.random.uniform(splits[10], (NZ,), jnp.float32, math.log(0.05), math.log(1.0))), 0.05, 1.0),
    }


def wash(conc):
    return conc * conc / (1.0 + conc * conc)


def slope(conc):
    denom = 1.0 + conc * conc
    return 2.0 * conc / (denom * denom)


def spread(padded, coefs):
    west_coef, east_coef, south_coef, north_coef, above_coef, below_coef, diag_coef = coefs
    total = diag_coef * padded[1:-1, 1:-1, 1:-1]
    total = total + west_coef * padded[1:-1, :-2, 1:-1] + east_coef * padded[1:-1, 2:, 1:-1]
    total = total + south_coef * padded[1:-1, 1:-1, :-2] + north_coef * padded[1:-1, 1:-1, 2:]
    total = total + above_coef * padded[2:, 1:-1, 1:-1] + below_coef * padded[:-2, 1:-1, 1:-1]
    return total


def reference(fields, slot_pick, courant_x, courant_y, horiz_diff, vert_diff, precip_class, class_rates, vent_cells, vent_rate, profile):
    start = fields[0, slot_pick[0]]
    lam_two = fields[1, slot_pick[1]]
    horiz = horiz_diff[:, None, None]
    vertical = vert_diff[:, None, None]
    zero_one = jnp.zeros((1,), jnp.float32)
    kd_above = jnp.concatenate([vert_diff[1:], zero_one])[:, None, None]
    kd_below = jnp.concatenate([zero_one, vert_diff[:-1]])[:, None, None]
    diag_coef = 1.0 - courant_x - courant_y - 4.0 * horiz - 2.0 * vertical
    cu_next = jnp.concatenate([courant_x[:, 1:, :], jnp.zeros((NZ, 1, NY), jnp.float32)], 1)
    cv_next = jnp.concatenate([courant_y[:, :, 1:], jnp.zeros((NZ, NX, 1), jnp.float32)], 2)
    flat_h = horiz + 0.0 * courant_x
    fwd_coefs = (courant_x + horiz, flat_h, courant_y + horiz, flat_h, vertical + 0.0 * courant_x, vertical + 0.0 * courant_x, diag_coef)
    adj_coefs = (flat_h, cu_next + horiz, flat_h, cv_next + horiz, kd_above + 0.0 * courant_x, kd_below + 0.0 * courant_x, diag_coef)
    rate = class_rates[precip_class]
    column = jnp.zeros((NX * NY,), jnp.float32).at[vent_cells].add(vent_rate).reshape(NX, NY)
    emission = profile[:, None, None] * column

    def padit(field):
        return jnp.pad(field, ((1, 1), (1, 1), (1, 1)))

    conc_one = spread(padit(start), fwd_coefs) - rate * wash(start) + emission
    conc_two = spread(padit(conc_one), fwd_coefs) - rate * wash(conc_one) + emission
    lam_one = spread(padit(lam_two), adj_coefs) - rate * slope(conc_one) * lam_two
    lam_zero = spread(padit(lam_one), adj_coefs) - rate * slope(start) * lam_one
    colsum = jnp.sum(profile[:, None, None] * (lam_one + lam_two), 0).reshape(-1)
    sensitivity = colsum[vent_cells]
    return jnp.stack([conc_two, lam_zero]), sensitivity
```

```python
import functools

import jax
import jax.numpy as jnp
from jax import lax
from jax.experimental import pallas as pl
from jax.experimental.pallas import tpu as pltpu
from jax.sharding import PartitionSpec as P

LANES = 128
SUBLANES = 8


def vmem():
    return pl.BlockSpec(memory_space=pltpu.VMEM)


def hbm():
    return pl.BlockSpec(memory_space=pltpu.HBM)


def neighbour(value, axis, by):
    size = lax.axis_size(axis)
    pairs = [(i, i + by) for i in range(size) if 0 <= i + by < size]
    return lax.ppermute(value, axis, pairs)


def doubling_steps():
    steps = []
    for axis in ("gx", "gy"):
        step = 1
        while step < lax.axis_size(axis):
            steps.append((axis, step))
            step *= 2
    return steps


def partner(value, axis, step):
    return lax.ppermute(value, axis, [(i, i ^ step) for i in range(lax.axis_size(axis))])


def inverse(conc):
    return 1.0 / (1.0 + conc * conc)


def wash(conc):
    return conc * conc * inverse(conc)


def slope(conc):
    inv = inverse(conc)
    return 2.0 * conc * inv * inv


def iotas(rows, cols):
    return (
        lax.broadcasted_iota(jnp.int32, (rows, cols), 0),
        lax.broadcasted_iota(jnp.int32, (rows, cols), 1),
    )


def wide(block, cols):
    return jnp.concatenate([block] * (cols // LANES), axis=1)


def lane_to(block, lane, target):
    return pltpu.roll(block, lax.rem(target - lane + 2 * LANES, LANES), 1)


def get_row(ref, r, lanes=slice(None)):
    base = pl.multiple_of((r // SUBLANES) * SUBLANES, SUBLANES)
    block = ref[pl.ds(base, SUBLANES), lanes]
    return pltpu.roll(block, lax.rem(SUBLANES - lax.rem(r, SUBLANES), SUBLANES), 0)[0:1]


def put_row(ref, r, value, lanes=slice(None)):
    base = pl.multiple_of((r // SUBLANES) * SUBLANES, SUBLANES)
    block = ref[pl.ds(base, SUBLANES), lanes]
    sub = lax.broadcasted_iota(jnp.int32, block.shape, 0)
    ref[pl.ds(base, SUBLANES), lanes] = jnp.where(sub == lax.rem(r, SUBLANES), value, block)


class Sides:
    def __init__(self, west, east, south, north):
        self.west, self.east, self.south, self.north = west, east, south, north


def level_coefs(adjoint, z, levels, horiz, vert):
    h = horiz[z]
    k = vert[z]
    if adjoint:
        above = vert[jnp.minimum(z + 1, levels - 1)]
        below = vert[jnp.maximum(z - 1, 0)]
    else:
        above = below = k
    above = jnp.where(z < levels - 1, above, 0.0)
    below = jnp.where(z > 0, below, 0.0)
    return h, k, above, below


def apply_plane(adjoint, z, levels, field, up, down, cu, cv, horiz, vert, sides):
    rows, cols = field.shape
    row, col = iotas(rows, cols)
    h, k, above, below = level_coefs(adjoint, z, levels, horiz, vert)
    if adjoint:
        to_east = (cu + h) * field
        to_north = (cv + h) * field
    else:
        to_east = to_north = h * field
    west = pltpu.roll(field, 1, 0)
    east = pltpu.roll(to_east, rows - 1, 0)
    south = pltpu.roll(field, 1, 1)
    north = pltpu.roll(to_north, cols - 1, 1)
    if sides is not None:
        west = jnp.where(row == 0, get_row(sides.west, z), west)
        east = jnp.where(row == rows - 1, get_row(sides.east, z), east)
        south = jnp.where(col == 0, wide(lane_to(sides.south[...], z, 0), cols), south)
        north = jnp.where(
            col == cols - 1, wide(lane_to(sides.north[...], z, LANES - 1), cols), north
        )
    diag = 1.0 - cu - cv - (4.0 * h + 2.0 * k)
    if adjoint:
        total = diag * field + h * (west + south) + east + north
    else:
        total = diag * field + (cu + h) * west + (cv + h) * south + east + north
    return total + above * up + below * down


def here_of(cells, v, dims):
    _, rows, cols, grid_y = dims
    x = cells[v] // grid_y - lax.axis_index("gx") * rows
    y = lax.rem(cells[v], grid_y) - lax.axis_index("gy") * cols
    return x, y, (x >= 0) & (x < rows) & (y >= 0) & (y < cols)


def gather_vents(cells, source, target, dims):
    levels = dims[0]
    _, lane = iotas(SUBLANES, LANES)

    def one(v, carry):
        x, y, here = here_of(cells, v, dims)

        @pl.when(here)
        def _():
            base = pl.multiple_of((y // LANES) * LANES, LANES)
            low = lax.rem(y, LANES)
            top = pl.multiple_of((x // SUBLANES) * SUBLANES, SUBLANES)
            got = jnp.zeros((SUBLANES, LANES), jnp.float32)
            for z in range(levels):
                block = source[z, pl.ds(top, SUBLANES), pl.ds(base, LANES)]
                got = jnp.where(lane == z, lane_to(block, low, z), got)
            got = pltpu.roll(got, lax.rem(SUBLANES - lax.rem(x, SUBLANES), SUBLANES), 0)[0:1]
            put_row(target, 2 * levels + v, got, slice(LANES, 2 * LANES))

        return carry

    lax.fori_loop(0, cells.shape[0], one, 0)


def gather_edges(source, target, dims):
    levels, rows, cols, _ = dims
    _, lane = iotas(rows, LANES)

    def group(i, columns):
        base = pl.multiple_of(i * SUBLANES, SUBLANES)
        for s in range(SUBLANES):
            z = base + s
            columns = jnp.where(lane == z, lane_to(source[z, :, 0:LANES], 0, z), columns)
            columns = jnp.where(
                lane == z + levels,
                lane_to(source[z, :, cols - LANES : cols], LANES - 1, z + levels),
                columns,
            )
        for top, row in ((0, 0), (levels, rows - 1)):
            lines = [source[base + s, row : row + 1, :] for s in range(SUBLANES)]
            at = pl.multiple_of(top + base, SUBLANES)
            target[pl.ds(at, SUBLANES), :] = jnp.concatenate(lines, axis=0)
        return columns

    zero = jnp.zeros((rows, LANES), jnp.float32)
    columns = lax.fori_loop(0, levels // SUBLANES, group, zero)
    target[2 * levels : 2 * levels + rows, 0:LANES] = columns


def head_kernel(slot_hbm, fields, out, slot, sems):
    copy = pltpu.make_async_copy(slot_hbm, slot, sems.at[0])
    copy.start()
    copy.wait()
    pick = slot[lax.axis_index("section")]
    copy = pltpu.make_async_copy(fields.at[0, pick, pl.ds(0, out.shape[0])], out, sems.at[1])
    copy.start()
    copy.wait()


def edges_kernel(
    dims,
    slot_hbm,
    horiz_hbm,
    class_hbm,
    cells_hbm,
    vent_hbm,
    fields,
    cu_hbm,
    cv_hbm,
    precip,
    out_xf,
    out_xb,
    out_yf,
    out_yb,
    out_cu0,
    out_cv0,
    out_rate,
    out_column,
    out_edges,
    out_edge_rate,
    slot,
    horiz,
    class_rates,
    cells,
    vent_rate,
    field,
    cu,
    cv,
    small_sems,
    sems,
):
    levels, rows, cols, _ = dims
    adj = lax.axis_index("section")
    flag = adj.astype(jnp.float32)
    courants = [
        pltpu.make_async_copy(cv_hbm.at[:, :, pl.ds(0, LANES)], cv, sems.at[1]),
        pltpu.make_async_copy(cu_hbm.at[:, pl.ds(0, SUBLANES), :], cu, sems.at[2]),
    ]
    small = [
        pltpu.make_async_copy(a, b, small_sems.at[i])
        for i, (a, b) in enumerate(
            (
                (slot_hbm, slot),
                (horiz_hbm, horiz),
                (class_hbm, class_rates),
                (cells_hbm, cells),
                (vent_hbm, vent_rate),
            )
        )
    ]
    for copy in small:
        copy.start()
    for copy in small:
        copy.wait()
    copies = [pltpu.make_async_copy(fields.at[0, slot[adj]], field, sems.at[0])] + courants
    for copy in copies:
        copy.start()

    kinds = precip[...]
    rate = jnp.zeros((rows, cols), jnp.float32)
    for kind in range(class_rates.shape[0]):
        rate = jnp.where(kinds == kind, class_rates[kind], rate)
    out_rate[...] = rate
    out_column[...] = jnp.zeros((rows, cols), jnp.float32)
    tail = slice(2 * levels, out_edges.shape[0])
    blank = jnp.zeros((out_edges.shape[0] - 2 * levels, cols), jnp.float32)
    out_edges[tail, :] = blank
    out_edge_rate[tail, :] = blank
    _, line_col = iotas(1, cols)

    def one(v, carry):
        x, y, here = here_of(cells, v, dims)

        @pl.when(here)
        def _():
            hit = line_col == y
            line = get_row(out_column, x) + jnp.where(hit, vent_rate[v], 0.0)
            put_row(out_column, x, line)
            found = jnp.sum(jnp.where(hit, get_row(out_rate, x), 0.0), axis=1, keepdims=True)
            found = jnp.broadcast_to(found, (1, LANES))
            put_row(out_edge_rate, 2 * levels + v, found, slice(LANES, 2 * LANES))

        return carry

    lax.fori_loop(0, cells.shape[0], one, 0)
    out_edge_rate[0:levels, :] = jnp.broadcast_to(rate[0:1, :], (levels, cols))
    out_edge_rate[levels : 2 * levels, :] = jnp.broadcast_to(rate[rows - 1 : rows, :], (levels, cols))
    _, lane = iotas(rows, LANES)
    out_edge_rate[2 * levels : 2 * levels + rows, 0:LANES] = jnp.where(
        lane < levels, rate[:, 0:1], rate[:, cols - 1 : cols]
    )

    copies[0].wait()
    gather_edges(field, out_edges, dims)
    gather_vents(cells, field, out_edges, dims)
    copies[1].wait()
    copies[2].wait()

    def group(i, columns):
        base = pl.multiple_of(i * SUBLANES, SUBLANES)
        lines = []
        for s in range(SUBLANES):
            z = base + s
            h = horiz[z]
            block = h + flag * cv[z]
            columns = jnp.where(lane == z, lane_to(block, 0, z), columns)
            lines.append(h + flag * cu[z, 0:1, :])
        out_cu0[pl.ds(base, SUBLANES), :] = jnp.concatenate(lines, axis=0)
        return columns

    zero = jnp.zeros((rows, LANES), jnp.float32)
    out_cv0[...] = lax.fori_loop(0, levels // SUBLANES, group, zero)
    columns = out_edges[2 * levels : 2 * levels + rows, 0:LANES]
    out_xf[...] = out_edges[levels : 2 * levels, :]
    out_xb[...] = out_cu0[...] * out_edges[0:levels, :]
    out_yf[...] = pltpu.roll(columns, LANES - levels, 1)
    out_yb[...] = out_cv0[...] * columns


def load_small(pairs, sems):
    copies = [pltpu.make_async_copy(a, b, sems.at[i]) for i, (a, b) in enumerate(pairs)]
    for copy in copies:
        copy.start()
    for copy in copies:
        copy.wait()


def first_kernel(
    dims,
    chunks,
    blocks,
    slot_hbm,
    horiz_hbm,
    vert_hbm,
    profile_hbm,
    cells_hbm,
    fields,
    cu_hbm,
    cv_hbm,
    west,
    east,
    south,
    north,
    rate,
    column,
    *rest,
):
    levels, _, cols, _ = dims
    out_pack, out_edges = rest[:2]
    out_chunks = rest[2 : 2 + len(chunks)]
    slot, horiz, vert, profile, cells = rest[2 + len(chunks) : 7 + len(chunks)]
    field, cu, cv, first, small_sems, in_sems, out_sems, chunk_sems = rest[7 + len(chunks) :]
    adj = lax.axis_index("section")
    size = levels // blocks
    spans = [pl.ds(b * size, size) for b in range(blocks)]
    loads = [
        [
            pltpu.make_async_copy(cu_hbm.at[span], cu.at[span], in_sems.at[b, 0]),
            pltpu.make_async_copy(cv_hbm.at[span], cv.at[span], in_sems.at[b, 1]),
        ]
        for b, span in enumerate(spans)
    ]
    for copy in loads[0]:
        copy.start()
    load_small(
        (
            (slot_hbm, slot),
            (horiz_hbm, horiz),
            (vert_hbm, vert),
            (profile_hbm, profile),
            (cells_hbm, cells),
        ),
        small_sems,
    )
    pick = slot[adj]
    for b, span in enumerate(spans):
        copy = pltpu.make_async_copy(fields.at[0, pick, span], field.at[span], in_sems.at[b, 2])
        copy.start()
        if b:
            for other in loads[b]:
                other.start()
        loads[b].append(copy)
    tail = slice(2 * levels, out_edges.shape[0])
    out_edges[tail, :] = jnp.zeros((out_edges.shape[0] - 2 * levels, cols), jnp.float32)
    sides = Sides(west, east, south, north)

    def planes(adjoint, low, high):
        def plane(z, carry):
            here = field[z]
            up = field[jnp.minimum(z + 1, levels - 1)]
            down = field[jnp.maximum(z - 1, 0)]
            value = apply_plane(
                adjoint, z, levels, here, up, down, cu[z], cv[z], horiz, vert, sides
            )
            if not adjoint:
                value = value - rate[...] * wash(here) + profile[z] * column[...]
            first[z] = value
            return carry

        lax.fori_loop(low, high, plane, 0)

    stores = []
    for copy in loads[0]:
        copy.wait()
    for b, span in enumerate(spans):
        if b + 1 < blocks:
            for copy in loads[b + 1]:
                copy.wait()
        low = b * size
        high = low + size

        @pl.when(adj == 0)
        def _():
            planes(False, low, high)

        @pl.when(adj == 1)
        def _():
            planes(True, low, high)

        for i, part in enumerate((first, cu, cv, field)):
            store = pltpu.make_async_copy(part.at[span], out_pack.at[span, i], out_sems.at[b, i])
            store.start()
            stores.append(store)
    for i, (low, high) in enumerate(chunks):
        span = pl.ds(low, high - low)
        store = pltpu.make_async_copy(field.at[span], out_chunks[i], chunk_sems.at[i])
        store.start()
        stores.append(store)
    gather_edges(first, out_edges, dims)
    gather_vents(cells, first, out_edges, dims)
    for store in stores:
        store.wait()


def rim_kernel(
    dims,
    profile,
    mine,
    theirs,
    edges,
    edge_rate,
    cu0,
    cv0,
    out_rim,
    out_xf,
    out_xb,
    out_yf,
    out_yb,
    out_terms,
):
    levels, rows, _, _ = dims
    adj = lax.axis_index("section")
    lam = mine[...] - edge_rate[...] * slope(theirs[...]) * edges[...]
    rim = jnp.where(adj == 1, lam, mine[...])
    out_rim[...] = rim
    columns = rim[2 * levels : 2 * levels + rows, 0:LANES]
    out_xf[...] = rim[levels : 2 * levels, :]
    out_xb[...] = cu0[...] * rim[0:levels, :]
    out_yf[...] = pltpu.roll(columns, LANES - levels, 1)
    out_yb[...] = cv0[...] * columns
    vents = out_terms.shape[1]
    at = slice(2 * levels, 2 * levels + vents)
    both = lam[at, LANES : 2 * LANES] + edges[at, LANES : 2 * LANES]
    weights = jnp.concatenate(
        [profile[...], jnp.zeros((1, LANES - levels), jnp.float32)], axis=1
    )
    both = jnp.concatenate([both * weights, jnp.zeros((LANES - vents, LANES), jnp.float32)], axis=0)
    sums = jnp.sum(jnp.transpose(both), axis=0, keepdims=True)[:, 0:vents]
    out_terms[...] = jnp.where(adj == 1, sums, 0.0)


def window_of(piece, levels):
    low, high = piece
    last = high == levels
    base = max(low - 3, 0)
    new0 = max(low - 1, 0)
    out0 = max(low - 2, 0)
    new1 = levels if last else high - 1
    out1 = levels if last else high - 2
    return base, (new0, new1), (out0, out1)


def load_kernel(base, pack, out, sem):
    copy = pltpu.make_async_copy(pack.at[pl.ds(base, out.shape[0])], out, sem.at[0])
    copy.start()
    copy.wait()


def chunk_kernel(
    dims,
    piece,
    following,
    horiz_hbm,
    vert_hbm,
    profile_hbm,
    pack,
    window,
    west,
    east,
    south,
    north,
    rate,
    column,
    rim,
    arrived,
    *rest,
):
    levels, rows, cols, _ = dims
    low, high = piece
    has_carry = low > 0
    if not following:
        terms, more_terms = rest[:2]
        rest = rest[2:]
    if has_carry:
        carry_in, _ = rest[:2]
        rest = rest[2:]
    out_hbm = rest[0]
    rest = rest[1:]
    if following:
        next_window, carry_out = rest[:2]
        rest = rest[2:]
    else:
        rest[0][...] = terms[...] + more_terms[...]
        rest = rest[1:]
    horiz, vert, profile, conc, fresh, result, small_sems, next_sem, out_sems = rest
    adj = lax.axis_index("section")
    base, (new0, new1), (out0, out1) = window_of(piece, levels)
    conc0 = out0
    sides = Sides(west, east, south, north)
    if following:
        start, _, _ = window_of(following, levels)
        ahead = pltpu.make_async_copy(
            pack.at[pl.ds(start, next_window.shape[0])], next_window, next_sem.at[0]
        )
        ahead.start()
    load_small(((horiz_hbm, horiz), (vert_hbm, vert), (profile_hbm, profile)), small_sems)

    def store(z):
        return pltpu.make_async_copy(
            result.at[z - out0], out_hbm.at[z], out_sems.at[z - out0]
        )

    @pl.when(adj == 1)
    def _():
        def move(z, carry):
            conc[low - conc0 + z] = arrived[z]
            return carry

        lax.fori_loop(0, high - low, move, 0)
        if has_carry:
            fresh[0:2] = carry_in[0:2]
            conc[0:2] = carry_in[2:4]

        def new_plane(z, carry):
            i = z - conc0
            j = z - base
            here = conc[i]
            up = conc[jnp.minimum(z + 1, levels - 1) - conc0]
            down = conc[jnp.maximum(z - 1, 0) - conc0]
            value = apply_plane(
                False, z, levels, here, up, down, window[j, 1], window[j, 2], horiz, vert, None
            )
            value = value - rate[...] * wash(here) + profile[z] * column[...]
            value = window[j, 0] - rate[...] * slope(value) * window[j, 3]
            row, col = iotas(rows, cols)
            columns = rim[2 * levels : 2 * levels + rows, 0:LANES]
            value = jnp.where(col == 0, wide(lane_to(columns, z, 0), cols), value)
            value = jnp.where(
                col == cols - 1, wide(lane_to(columns, z + levels, LANES - 1), cols), value
            )
            value = jnp.where(row == 0, get_row(rim, z), value)
            value = jnp.where(row == rows - 1, get_row(rim, levels + z), value)
            fresh[j] = value
            return carry

        lax.fori_loop(new0, new1, new_plane, 0)
        if following:
            carry_out[0:2] = fresh[new1 - 2 - base : new1 - base]
            carry_out[2:4] = conc[high - 2 - conc0 : high - conc0]

        def out_plane(z, carry):
            j = z - base
            here = fresh[j]
            up = fresh[jnp.minimum(z + 1, levels - 1) - base]
            down = fresh[jnp.maximum(z - 1, 0) - base]
            value = apply_plane(
                True, z, levels, here, up, down, window[j, 1], window[j, 2], horiz, vert, sides
            )
            result[z - out0] = value - rate[...] * slope(conc[z - conc0]) * here
            store(z).start()
            return carry

        lax.fori_loop(out0, out1, out_plane, 0)

    @pl.when(adj == 0)
    def _():
        def out_plane(z, carry):
            j = z - base
            here = window[j, 0]
            up = window[jnp.minimum(z + 1, levels - 1) - base, 0]
            down = window[jnp.maximum(z - 1, 0) - base, 0]
            value = apply_plane(
                False, z, levels, here, up, down, window[j, 1], window[j, 2], horiz, vert, sides
            )
            result[z - out0] = value - rate[...] * wash(here) + profile[z] * column[...]
            store(z).start()
            return carry

        lax.fori_loop(out0, out1, out_plane, 0)

    def wait(z, carry):
        store(z).wait()
        return carry

    lax.fori_loop(out0, out1, wait, 0)
    if following:
        ahead.wait()


def cost(cells, ops, arrays):
    return pl.CostEstimate(flops=cells * ops, bytes_accessed=4 * cells * arrays, transcendentals=0)


def cuts(levels):
    unit = levels // 16
    sizes = [5 * unit, 4 * unit, 4 * unit, 2 * unit, levels - 15 * unit]
    bounds = [0]
    for size in sizes:
        bounds.append(bounds[-1] + size)
    return list(zip(bounds[:-1], bounds[1:]))


def program(
    fields,
    slot_pick,
    courant_x,
    courant_y,
    horiz_diff,
    vert_diff,
    precip_class,
    class_rates,
    vent_cells,
    vent_rate,
    profile,
):
    levels, rows, cols = courant_x.shape
    vents = vent_cells.shape[0]
    grid_y = cols * lax.axis_size("gy")
    dims = (levels, rows, cols, grid_y)
    cells = levels * rows * cols
    edge_rows = 2 * levels + max(rows, vents)
    f32 = jnp.float32
    i32 = jnp.int32
    shape = jax.ShapeDtypeStruct
    full = shape((levels, rows, cols), f32)
    line = shape((levels, cols), f32)
    side = shape((rows, LANES), f32)
    flat = shape((rows, cols), f32)
    rims = shape((edge_rows, cols), f32)
    pieces = cuts(levels)

    whole_vmem = pltpu.CompilerParams(vmem_limit_bytes=58 * 1024 * 1024)
    params = pltpu.CompilerParams(vmem_limit_bytes=45 * 1024 * 1024)

    def send(value):
        return neighbour(value, "section", 1)

    low, high = pieces[0]
    start = pl.pallas_call(
        head_kernel,
        name="head",
        in_specs=[hbm()] * 2,
        out_specs=vmem(),
        out_shape=shape((high - low, rows, cols), f32),
        scratch_shapes=[pltpu.SMEM(slot_pick.shape, i32), pltpu.SemaphoreType.DMA((2,))],
        compiler_params=params,
        cost_estimate=cost(cells, 1, 1),
    )(slot_pick, fields)
    received = [send(start)]

    xf, xb, yf, yb, cu0, cv0, rate, column, edges, edge_rate = pl.pallas_call(
        functools.partial(edges_kernel, dims),
        name="edges",
        in_specs=[hbm()] * 8 + [vmem()],
        out_specs=[vmem()] * 10,
        out_shape=[line, line, side, side, line, side, flat, flat, rims, rims],
        scratch_shapes=[
            pltpu.SMEM(slot_pick.shape, i32),
            pltpu.SMEM(horiz_diff.shape, f32),
            pltpu.SMEM(class_rates.shape, f32),
            pltpu.SMEM(vent_cells.shape, i32),
            pltpu.SMEM(vent_rate.shape, f32),
            pltpu.VMEM(full.shape, f32),
            pltpu.VMEM((levels, SUBLANES, cols), f32),
            pltpu.VMEM((levels, rows, LANES), f32),
            pltpu.SemaphoreType.DMA((5,)),
            pltpu.SemaphoreType.DMA((3,)),
        ],
        compiler_params=whole_vmem,
        cost_estimate=cost(cells, 10, 2),
    )(
        slot_pick, horiz_diff, class_rates, vent_cells, vent_rate,
        fields, courant_x, courant_y, precip_class,
    )

    west = neighbour(xf, "gx", 1)
    east = neighbour(xb, "gx", -1)
    south = neighbour(yf, "gy", 1)
    north = neighbour(yb, "gy", -1)

    levels_smem = [pltpu.SMEM((levels,), f32)] * 3
    blocks = 4
    pack, mine, *later = pl.pallas_call(
        functools.partial(first_kernel, dims, pieces[1:], blocks),
        name="first",
        in_specs=[hbm()] * 8 + [vmem()] * 6,
        out_specs=[hbm(), vmem()] + [hbm()] * (len(pieces) - 1),
        out_shape=[shape((levels, 4, rows, cols), f32), rims]
        + [shape((b - a, rows, cols), f32) for a, b in pieces[1:]],
        scratch_shapes=[pltpu.SMEM(slot_pick.shape, i32)]
        + levels_smem
        + [pltpu.SMEM(vent_cells.shape, i32)]
        + [pltpu.VMEM(full.shape, f32)] * 4
        + [
            pltpu.SemaphoreType.DMA((5,)),
            pltpu.SemaphoreType.DMA((blocks, 3)),
            pltpu.SemaphoreType.DMA((blocks, 4)),
            pltpu.SemaphoreType.DMA((len(pieces) - 1,)),
        ],
        compiler_params=whole_vmem,
        cost_estimate=cost(cells, 40, 5),
    )(
        slot_pick, horiz_diff, vert_diff, profile, vent_cells,
        fields, courant_x, courant_y, west, east, south, north, rate, column,
    )

    theirs = send(mine)
    for piece in later:
        received.append(send(piece))

    rim, xf, xb, yf, yb, terms = pl.pallas_call(
        functools.partial(rim_kernel, dims),
        name="rim",
        in_specs=[vmem()] * 7,
        out_specs=[vmem()] * 6,
        out_shape=[rims, line, line, side, side, shape((1, vents), f32)],
        compiler_params=params,
        cost_estimate=cost(edge_rows * cols, 20, 5),
    )(profile[None, :], mine, theirs, edges, edge_rate, cu0, cv0)
    west = neighbour(xf, "gx", 1)
    east = neighbour(xb, "gx", -1)
    south = neighbour(yf, "gy", 1)
    north = neighbour(yb, "gy", -1)

    def load_window(piece):
        base, (_, end), _ = window_of(piece, levels)
        return shape((end - base, 4, rows, cols), f32)

    window = pl.pallas_call(
        functools.partial(load_kernel, window_of(pieces[0], levels)[0]),
        name="load",
        in_specs=[hbm()],
        out_specs=vmem(),
        out_shape=load_window(pieces[0]),
        scratch_shapes=[pltpu.SemaphoreType.DMA((1,))],
        compiler_params=params,
        cost_estimate=cost(cells, 10, 1),
    )(pack)

    terms = terms + lax.ppermute(terms, "section", [(1, 0)])
    steps = doubling_steps()
    while len(steps) > len(pieces) - 1:
        terms = terms + partner(terms, *steps.pop(0))

    result = carry = None
    more = jnp.zeros_like(terms)
    for j, piece in enumerate(pieces):
        low, high = piece
        following = pieces[j + 1] if j + 1 < len(pieces) else None
        base, (_, end), (out0, out1) = window_of(piece, levels)
        outs = out1 - out0
        if following and steps:
            more = partner(terms, *steps.pop(0))
        operands = [
            horiz_diff, vert_diff, profile, pack, window,
            west, east, south, north, rate, column, rim, received[j],
        ]
        specs = [hbm()] * 4 + [vmem()] * 9
        aliases = {}
        if not following:
            operands += [terms, more]
            specs += [vmem()] * 2
        if low > 0:
            operands += [carry, result]
            specs += [vmem(), hbm()]
            aliases = {len(operands) - 1: 0}
        out_shape = [full]
        out_specs = [hbm()]
        if following:
            out_shape += [load_window(following), shape((4, rows, cols), f32)]
            out_specs += [vmem(), vmem()]
        else:
            out_shape += [shape((1, vents), f32)]
            out_specs += [vmem()]
        result, *state = pl.pallas_call(
            functools.partial(chunk_kernel, dims, piece, following),
            in_specs=specs,
            out_specs=out_specs,
            out_shape=out_shape,
            scratch_shapes=levels_smem
            + [
                pltpu.VMEM((high - out0, rows, cols), f32),
                pltpu.VMEM((end - base, rows, cols), f32),
                pltpu.VMEM((outs, rows, cols), f32),
                pltpu.SemaphoreType.DMA((3,)),
                pltpu.SemaphoreType.DMA((1,)),
                pltpu.SemaphoreType.DMA((outs,)),
            ],
            input_output_aliases=aliases,
            compiler_params=params,
            cost_estimate=cost((high - low) * rows * cols, 80, 7),
        )(*operands)
        if following:
            window, carry = state
            if steps:
                terms = terms + more
                more = jnp.zeros_like(terms)
        else:
            (terms,) = state
    return (result[None], terms[0])


def solution(mesh):
    return jax.shard_map(
        program,
        mesh=mesh,
        in_specs=(
            P("section", None, None, "gx", "gy"),
            P(),
            P(None, "gx", "gy"),
            P(None, "gx", "gy"),
            P(),
            P(),
            P("gx", "gy"),
            P(),
            P(),
            P(),
            P(),
        ),
        out_specs=(P("section", None, "gx", "gy"), P()),
        check_vma=False,
    )
```

```python
import functools

import jax
import jax.numpy as jnp
from jax import lax
from jax.experimental import pallas as pl
from jax.experimental.pallas import tpu as pltpu
from jax.sharding import PartitionSpec as P

LANES = 128
SUBLANES = 8
SLOTS = 7


def vmem():
    return pl.BlockSpec(memory_space=pltpu.VMEM)


def hbm():
    return pl.BlockSpec(memory_space=pltpu.HBM)


def neighbour(value, axis, by):
    size = lax.axis_size(axis)
    pairs = [(i, i + by) for i in range(size) if 0 <= i + by < size]
    return lax.ppermute(value, axis, pairs)


def doubling_steps():
    wide, deep = lax.axis_size("gx"), lax.axis_size("gy")
    steps = []
    step = 1
    while step < wide * deep:
        steps.append([(i, i ^ step) for i in range(wide * deep)])
        step *= 2
    return steps


def partner(value, pairs):
    return lax.ppermute(value, ("section", "gx", "gy"), pairs)


def inverse(conc):
    return 1.0 / (1.0 + conc * conc)


def wash(conc):
    return conc * conc * inverse(conc)


def slope(conc):
    inv = inverse(conc)
    return 2.0 * conc * inv * inv


def iotas(rows, cols):
    return (
        lax.broadcasted_iota(jnp.int32, (rows, cols), 0),
        lax.broadcasted_iota(jnp.int32, (rows, cols), 1),
    )


def wide(block, cols):
    return jnp.concatenate([block] * (cols // LANES), axis=1)


def lane_to(block, lane, target):
    return pltpu.roll(block, lax.rem(target - lane + 2 * LANES, LANES), 1)


def get_row(ref, r, lanes=slice(None)):
    base = pl.multiple_of((r // SUBLANES) * SUBLANES, SUBLANES)
    block = ref[pl.ds(base, SUBLANES), lanes]
    return pltpu.roll(block, lax.rem(SUBLANES - lax.rem(r, SUBLANES), SUBLANES), 0)[0:1]


def put_row(ref, r, value, lanes=slice(None)):
    base = pl.multiple_of((r // SUBLANES) * SUBLANES, SUBLANES)
    block = ref[pl.ds(base, SUBLANES), lanes]
    sub = lax.broadcasted_iota(jnp.int32, block.shape, 0)
    ref[pl.ds(base, SUBLANES), lanes] = jnp.where(sub == lax.rem(r, SUBLANES), value, block)


class Sides:
    def __init__(self, west, east, south, north):
        self.west, self.east, self.south, self.north = west, east, south, north


def level_coefs(adjoint, z, levels, horiz, vert):
    h = horiz[z]
    k = vert[z]
    if adjoint:
        above = vert[jnp.minimum(z + 1, levels - 1)]
        below = vert[jnp.maximum(z - 1, 0)]
    else:
        above = below = k
    above = jnp.where(z < levels - 1, above, 0.0)
    below = jnp.where(z > 0, below, 0.0)
    return h, k, above, below


def apply_plane(adjoint, z, levels, field, up, down, cu, cv, horiz, vert, sides):
    rows, cols = field.shape
    row, col = iotas(rows, cols)
    h, k, above, below = level_coefs(adjoint, z, levels, horiz, vert)
    if adjoint:
        to_east = (cu + h) * field
        to_north = (cv + h) * field
    else:
        to_east = to_north = h * field
    west = pltpu.roll(field, 1, 0)
    east = pltpu.roll(to_east, rows - 1, 0)
    south = pltpu.roll(field, 1, 1)
    north = pltpu.roll(to_north, cols - 1, 1)
    if sides is not None:
        west = jnp.where(row == 0, get_row(sides.west, z), west)
        east = jnp.where(row == rows - 1, get_row(sides.east, z), east)
        south = jnp.where(col == 0, wide(lane_to(sides.south[...], z, 0), cols), south)
        north = jnp.where(
            col == cols - 1, wide(lane_to(sides.north[...], z, LANES - 1), cols), north
        )
    diag = 1.0 - cu - cv - (4.0 * h + 2.0 * k)
    if adjoint:
        total = diag * field + h * (west + south) + east + north
    else:
        total = diag * field + (cu + h) * west + (cv + h) * south + east + north
    return total + above * up + below * down


def here_of(cells, v, dims):
    _, rows, cols, grid_y = dims
    x = cells[v] // grid_y - lax.axis_index("gx") * rows
    y = lax.rem(cells[v], grid_y) - lax.axis_index("gy") * cols
    return x, y, (x >= 0) & (x < rows) & (y >= 0) & (y < cols)


def gather_vents(cells, source, target, dims):
    levels = dims[0]
    _, lane = iotas(SUBLANES, LANES)

    def one(v, carry):
        x, y, here = here_of(cells, v, dims)

        @pl.when(here)
        def _():
            base = pl.multiple_of((y // LANES) * LANES, LANES)
            low = lax.rem(y, LANES)
            top = pl.multiple_of((x // SUBLANES) * SUBLANES, SUBLANES)
            got = jnp.zeros((SUBLANES, LANES), jnp.float32)
            for z in range(levels):
                block = source[z, pl.ds(top, SUBLANES), pl.ds(base, LANES)]
                got = jnp.where(lane == z, lane_to(block, low, z), got)
            got = pltpu.roll(got, lax.rem(SUBLANES - lax.rem(x, SUBLANES), SUBLANES), 0)[0:1]
            put_row(target, 2 * levels + v, got, slice(LANES, 2 * LANES))

        return carry

    lax.fori_loop(0, cells.shape[0], one, 0)


def gather_edges(source, target, dims):
    levels, rows, cols, _ = dims
    _, lane = iotas(rows, LANES)

    def group(i, columns):
        base = pl.multiple_of(i * SUBLANES, SUBLANES)
        for s in range(SUBLANES):
            z = base + s
            columns = jnp.where(lane == z, lane_to(source[z, :, 0:LANES], 0, z), columns)
            columns = jnp.where(
                lane == z + levels,
                lane_to(source[z, :, cols - LANES : cols], LANES - 1, z + levels),
                columns,
            )
        for top, row in ((0, 0), (levels, rows - 1)):
            lines = [source[base + s, row : row + 1, :] for s in range(SUBLANES)]
            at = pl.multiple_of(top + base, SUBLANES)
            target[pl.ds(at, SUBLANES), :] = jnp.concatenate(lines, axis=0)
        return columns

    zero = jnp.zeros((rows, LANES), jnp.float32)
    columns = lax.fori_loop(0, levels // SUBLANES, group, zero)
    target[2 * levels : 2 * levels + rows, 0:LANES] = columns


def head_kernel(slot_hbm, fields, out, slot, sems):
    copy = pltpu.make_async_copy(slot_hbm, slot, sems.at[0])
    copy.start()
    copy.wait()
    pick = slot[lax.axis_index("section")]
    copy = pltpu.make_async_copy(fields.at[0, pick, pl.ds(0, out.shape[0])], out, sems.at[1])
    copy.start()
    copy.wait()


def edges_kernel(
    dims,
    slot_hbm,
    horiz_hbm,
    class_hbm,
    cells_hbm,
    vent_hbm,
    fields,
    cu_hbm,
    cv_hbm,
    precip,
    out_xf,
    out_xb,
    out_yf,
    out_yb,
    out_cu0,
    out_cv0,
    out_rate,
    out_column,
    out_edges,
    out_edge_rate,
    slot,
    horiz,
    class_rates,
    cells,
    vent_rate,
    field,
    cu,
    cv,
    small_sems,
    sems,
):
    levels, rows, cols, _ = dims
    adj = lax.axis_index("section")
    flag = adj.astype(jnp.float32)
    courants = [
        pltpu.make_async_copy(cv_hbm.at[:, :, pl.ds(0, LANES)], cv, sems.at[1]),
        pltpu.make_async_copy(cu_hbm.at[:, pl.ds(0, SUBLANES), :], cu, sems.at[2]),
    ]
    small = [
        pltpu.make_async_copy(a, b, small_sems.at[i])
        for i, (a, b) in enumerate(
            (
                (slot_hbm, slot),
                (horiz_hbm, horiz),
                (class_hbm, class_rates),
                (cells_hbm, cells),
                (vent_hbm, vent_rate),
            )
        )
    ]
    for copy in small:
        copy.start()
    for copy in small:
        copy.wait()
    copies = [pltpu.make_async_copy(fields.at[0, slot[adj]], field, sems.at[0])] + courants
    for copy in copies:
        copy.start()

    kinds = precip[...]
    rate = jnp.zeros((rows, cols), jnp.float32)
    for kind in range(class_rates.shape[0]):
        rate = jnp.where(kinds == kind, class_rates[kind], rate)
    out_rate[...] = rate
    out_column[...] = jnp.zeros((rows, cols), jnp.float32)
    tail = slice(2 * levels, out_edges.shape[0])
    blank = jnp.zeros((out_edges.shape[0] - 2 * levels, cols), jnp.float32)
    out_edges[tail, :] = blank
    out_edge_rate[tail, :] = blank
    _, line_col = iotas(1, cols)

    def one(v, carry):
        x, y, here = here_of(cells, v, dims)

        @pl.when(here)
        def _():
            hit = line_col == y
            line = get_row(out_column, x) + jnp.where(hit, vent_rate[v], 0.0)
            put_row(out_column, x, line)
            found = jnp.sum(jnp.where(hit, get_row(out_rate, x), 0.0), axis=1, keepdims=True)
            found = jnp.broadcast_to(found, (1, LANES))
            put_row(out_edge_rate, 2 * levels + v, found, slice(LANES, 2 * LANES))

        return carry

    lax.fori_loop(0, cells.shape[0], one, 0)
    out_edge_rate[0:levels, :] = jnp.broadcast_to(rate[0:1, :], (levels, cols))
    out_edge_rate[levels : 2 * levels, :] = jnp.broadcast_to(rate[rows - 1 : rows, :], (levels, cols))
    _, lane = iotas(rows, LANES)
    out_edge_rate[2 * levels : 2 * levels + rows, 0:LANES] = jnp.where(
        lane < levels, rate[:, 0:1], rate[:, cols - 1 : cols]
    )

    copies[0].wait()
    gather_edges(field, out_edges, dims)
    gather_vents(cells, field, out_edges, dims)
    copies[1].wait()
    copies[2].wait()

    def group(i, columns):
        base = pl.multiple_of(i * SUBLANES, SUBLANES)
        lines = []
        for s in range(SUBLANES):
            z = base + s
            h = horiz[z]
            block = h + flag * cv[z]
            columns = jnp.where(lane == z, lane_to(block, 0, z), columns)
            lines.append(h + flag * cu[z, 0:1, :])
        out_cu0[pl.ds(base, SUBLANES), :] = jnp.concatenate(lines, axis=0)
        return columns

    zero = jnp.zeros((rows, LANES), jnp.float32)
    out_cv0[...] = lax.fori_loop(0, levels // SUBLANES, group, zero)
    columns = out_edges[2 * levels : 2 * levels + rows, 0:LANES]
    out_xf[...] = out_edges[levels : 2 * levels, :]
    out_xb[...] = out_cu0[...] * out_edges[0:levels, :]
    out_yf[...] = pltpu.roll(columns, LANES - levels, 1)
    out_yb[...] = out_cv0[...] * columns


def load_small(pairs, sems):
    copies = [pltpu.make_async_copy(a, b, sems.at[i]) for i, (a, b) in enumerate(pairs)]
    for copy in copies:
        copy.start()
    for copy in copies:
        copy.wait()


def first_kernel(
    dims,
    chunks,
    blocks,
    slot_hbm,
    horiz_hbm,
    vert_hbm,
    profile_hbm,
    cells_hbm,
    fields,
    cu_hbm,
    cv_hbm,
    west,
    east,
    south,
    north,
    rate,
    column,
    edges,
    *rest,
):
    levels, _, cols, _ = dims
    out_pack, out_edges, out_vents = rest[:3]
    out_chunks = rest[3 : 3 + len(chunks)]
    slot, horiz, vert, profile, cells = rest[3 + len(chunks) : 8 + len(chunks)]
    field, cu, cv, first, small_sems, in_sems, out_sems, chunk_sems = rest[8 + len(chunks) :]
    adj = lax.axis_index("section")
    size = levels // blocks
    spans = [pl.ds(b * size, size) for b in range(blocks)]
    loads = [
        [
            pltpu.make_async_copy(cu_hbm.at[span], cu.at[span], in_sems.at[b, 0]),
            pltpu.make_async_copy(cv_hbm.at[span], cv.at[span], in_sems.at[b, 1]),
        ]
        for b, span in enumerate(spans)
    ]
    for copy in loads[0]:
        copy.start()
    load_small(
        (
            (slot_hbm, slot),
            (horiz_hbm, horiz),
            (vert_hbm, vert),
            (profile_hbm, profile),
            (cells_hbm, cells),
        ),
        small_sems,
    )
    pick = slot[adj]
    for b, span in enumerate(spans):
        copy = pltpu.make_async_copy(fields.at[0, pick, span], field.at[span], in_sems.at[b, 2])
        copy.start()
        if b:
            for other in loads[b]:
                other.start()
        loads[b].append(copy)
    tail = slice(2 * levels, out_edges.shape[0])
    out_edges[tail, :] = jnp.zeros((out_edges.shape[0] - 2 * levels, cols), jnp.float32)
    sides = Sides(west, east, south, north)

    def planes(adjoint, low, high):
        def plane(z, carry):
            here = field[z]
            up = field[jnp.minimum(z + 1, levels - 1)]
            down = field[jnp.maximum(z - 1, 0)]
            value = apply_plane(
                adjoint, z, levels, here, up, down, cu[z], cv[z], horiz, vert, sides
            )
            if not adjoint:
                value = value - rate[...] * wash(here) + profile[z] * column[...]
            first[z] = value
            return carry

        lax.fori_loop(low, high, plane, 0)

    stores = []
    for copy in loads[0]:
        copy.wait()
    for b, span in enumerate(spans):
        if b + 1 < blocks:
            for copy in loads[b + 1]:
                copy.wait()
        low = b * size
        high = low + size

        @pl.when(adj == 0)
        def _():
            planes(False, low, high)

        @pl.when(adj == 1)
        def _():
            planes(True, low, high)

        for i, part in enumerate((first, cu, cv, field)):
            store = pltpu.make_async_copy(part.at[span], out_pack.at[span, i], out_sems.at[b, i])
            store.start()
            stores.append(store)
    for i, (low, high) in enumerate(chunks):
        span = pl.ds(low, high - low)
        store = pltpu.make_async_copy(field.at[span], out_chunks[i], chunk_sems.at[i])
        store.start()
        stores.append(store)
    gather_edges(first, out_edges, dims)
    gather_vents(cells, first, out_edges, dims)
    at = slice(2 * levels, 2 * levels + out_vents.shape[0])
    out_vents[:, 0:LANES] = out_edges[at, LANES : 2 * LANES]
    out_vents[:, LANES : 2 * LANES] = edges[at, LANES : 2 * LANES]
    for store in stores:
        store.wait()


def rim_kernel(
    dims,
    profile,
    mine,
    theirs,
    at_vents,
    edges,
    edge_rate,
    cu0,
    cv0,
    out_rim,
    out_xf,
    out_xb,
    out_yf,
    out_yb,
    out_terms,
):
    levels, rows, _, _ = dims
    adj = lax.axis_index("section")
    lam = mine[...] - edge_rate[...] * slope(theirs[...]) * edges[...]
    rim = jnp.where(adj == 1, lam, mine[...])
    out_rim[...] = rim
    columns = rim[2 * levels : 2 * levels + rows, 0:LANES]
    out_xf[...] = rim[levels : 2 * levels, :]
    out_xb[...] = cu0[...] * rim[0:levels, :]
    out_yf[...] = pltpu.roll(columns, LANES - levels, 1)
    out_yb[...] = cv0[...] * columns
    vents = out_terms.shape[1]
    at = slice(2 * levels, 2 * levels + vents)
    right = slice(LANES, 2 * LANES)
    lam_two = at_vents[:, right]
    loss = edge_rate[at, right] * slope(mine[at, right]) * lam_two
    both = at_vents[:, 0:LANES] - loss + lam_two
    weights = jnp.concatenate(
        [profile[...], jnp.zeros((1, LANES - levels), jnp.float32)], axis=1
    )
    both = jnp.concatenate([both * weights, jnp.zeros((LANES - vents, LANES), jnp.float32)], axis=0)
    sums = jnp.sum(jnp.transpose(both), axis=0, keepdims=True)[:, 0:vents]
    out_terms[...] = sums


def window_of(piece, levels):
    low, high = piece
    last = high == levels
    base = max(low - 3, 0)
    new0 = max(low - 1, 0)
    out0 = max(low - 2, 0)
    new1 = levels if last else high - 1
    out1 = levels if last else high - 2
    return base, (new0, new1), (out0, out1)


def load_kernel(base, pack, out, sem):
    copy = pltpu.make_async_copy(
        pack.at[pl.ds(base, out.shape[0]), pl.ds(0, 4)], out, sem.at[0]
    )
    copy.start()
    copy.wait()


def chunk_kernel(
    dims,
    piece,
    following,
    horiz_hbm,
    vert_hbm,
    profile_hbm,
    pack,
    window,
    west,
    east,
    south,
    north,
    rate,
    column,
    rim,
    arrived,
    *rest,
):
    levels, rows, cols, _ = dims
    low, high = piece
    has_carry = low > 0
    if not following:
        terms, more_terms = rest[:2]
        rest = rest[2:]
    if has_carry:
        carry_in, _ = rest[:2]
        rest = rest[2:]
    out_hbm = rest[0]
    rest = rest[1:]
    if following:
        next_window, carry_out = rest[:2]
        rest = rest[2:]
    else:
        rest[0][...] = jnp.where(lax.axis_index("section") == 1, more_terms[...], terms[...])
        rest = rest[1:]
    horiz, vert, profile, conc, fresh, result, small_sems, next_sem, out_sems = rest
    adj = lax.axis_index("section")
    base, (new0, new1), (out0, out1) = window_of(piece, levels)
    conc0 = out0
    sides = Sides(west, east, south, north)
    if following:
        start, _, _ = window_of(following, levels)
        ahead = pltpu.make_async_copy(
            pack.at[pl.ds(start, next_window.shape[0]), pl.ds(0, 4)], next_window, next_sem.at[0]
        )
        ahead.start()
    load_small(((horiz_hbm, horiz), (vert_hbm, vert), (profile_hbm, profile)), small_sems)

    def store(z):
        return pltpu.make_async_copy(
            result.at[z - out0], out_hbm.at[z], out_sems.at[z - out0]
        )

    @pl.when(adj == 1)
    def _():
        def move(z, carry):
            conc[low - conc0 + z] = arrived[z]
            return carry

        lax.fori_loop(0, high - low, move, 0)
        if has_carry:
            fresh[0:2] = carry_in[0:2]
            conc[0:2] = carry_in[2:4]

        def new_plane(z, carry):
            i = z - conc0
            j = z - base
            here = conc[i]
            up = conc[jnp.minimum(z + 1, levels - 1) - conc0]
            down = conc[jnp.maximum(z - 1, 0) - conc0]
            value = apply_plane(
                False, z, levels, here, up, down, window[j, 1], window[j, 2], horiz, vert, None
            )
            value = value - rate[...] * wash(here) + profile[z] * column[...]
            value = window[j, 0] - rate[...] * slope(value) * window[j, 3]
            row, col = iotas(rows, cols)
            columns = rim[2 * levels : 2 * levels + rows, 0:LANES]
            value = jnp.where(col == 0, wide(lane_to(columns, z, 0), cols), value)
            value = jnp.where(
                col == cols - 1, wide(lane_to(columns, z + levels, LANES - 1), cols), value
            )
            value = jnp.where(row == 0, get_row(rim, z), value)
            value = jnp.where(row == rows - 1, get_row(rim, levels + z), value)
            fresh[j] = value
            return carry

        lax.fori_loop(new0, new1, new_plane, 0)
        if following:
            carry_out[0:2] = fresh[new1 - 2 - base : new1 - base]
            carry_out[2:4] = conc[high - 2 - conc0 : high - conc0]

        def out_plane(z, carry):
            j = z - base
            here = fresh[j]
            up = fresh[jnp.minimum(z + 1, levels - 1) - base]
            down = fresh[jnp.maximum(z - 1, 0) - base]
            value = apply_plane(
                True, z, levels, here, up, down, window[j, 1], window[j, 2], horiz, vert, sides
            )
            result[z - out0] = value - rate[...] * slope(conc[z - conc0]) * here
            store(z).start()
            return carry

        lax.fori_loop(out0, out1, out_plane, 0)

    @pl.when(adj == 0)
    def _():
        def out_plane(z, carry):
            j = z - base
            here = window[j, 0]
            up = window[jnp.minimum(z + 1, levels - 1) - base, 0]
            down = window[jnp.maximum(z - 1, 0) - base, 0]
            value = apply_plane(
                False, z, levels, here, up, down, window[j, 1], window[j, 2], horiz, vert, sides
            )
            result[z - out0] = value - rate[...] * wash(here) + profile[z] * column[...]
            store(z).start()
            return carry

        lax.fori_loop(out0, out1, out_plane, 0)

    def wait(z, carry):
        store(z).wait()
        return carry

    lax.fori_loop(out0, out1, wait, 0)
    if following:
        ahead.wait()


def cost(cells, ops, arrays):
    return pl.CostEstimate(flops=cells * ops, bytes_accessed=4 * cells * arrays, transcendentals=0)


def cuts(levels):
    sizes = [levels * part // 64 for part in (28, 16, 12, 6)]
    sizes.append(levels - sum(sizes))
    bounds = [0]
    for size in sizes:
        bounds.append(bounds[-1] + size)
    return list(zip(bounds[:-1], bounds[1:]))


def program(
    fields,
    slot_pick,
    courant_x,
    courant_y,
    horiz_diff,
    vert_diff,
    precip_class,
    class_rates,
    vent_cells,
    vent_rate,
    profile,
):
    levels, rows, cols = courant_x.shape
    vents = vent_cells.shape[0]
    grid_y = cols * lax.axis_size("gy")
    dims = (levels, rows, cols, grid_y)
    cells = levels * rows * cols
    edge_rows = 2 * levels + max(rows, vents)
    f32 = jnp.float32
    i32 = jnp.int32
    shape = jax.ShapeDtypeStruct
    full = shape((levels, rows, cols), f32)
    line = shape((levels, cols), f32)
    side = shape((rows, LANES), f32)
    flat = shape((rows, cols), f32)
    rims = shape((edge_rows, cols), f32)
    pieces = cuts(levels)

    whole_vmem = pltpu.CompilerParams(vmem_limit_bytes=58 * 1024 * 1024)
    params = pltpu.CompilerParams(vmem_limit_bytes=34 * 1024 * 1024)
    head_params = pltpu.CompilerParams(vmem_limit_bytes=45 * 1024 * 1024)

    def send(value):
        return neighbour(value, "section", 1)

    low, high = pieces[0]
    start = pl.pallas_call(
        head_kernel,
        name="head",
        in_specs=[hbm()] * 2,
        out_specs=vmem(),
        out_shape=shape((high - low, rows, cols), f32),
        scratch_shapes=[pltpu.SMEM(slot_pick.shape, i32), pltpu.SemaphoreType.DMA((2,))],
        compiler_params=head_params,
        cost_estimate=cost(cells, 1, 1),
    )(slot_pick, fields)
    received = [send(start)]

    xf, xb, yf, yb, cu0, cv0, rate, column, edges, edge_rate = pl.pallas_call(
        functools.partial(edges_kernel, dims),
        name="edges",
        in_specs=[hbm()] * 8 + [vmem()],
        out_specs=[vmem()] * 10,
        out_shape=[line, line, side, side, line, side, flat, flat, rims, rims],
        scratch_shapes=[
            pltpu.SMEM(slot_pick.shape, i32),
            pltpu.SMEM(horiz_diff.shape, f32),
            pltpu.SMEM(class_rates.shape, f32),
            pltpu.SMEM(vent_cells.shape, i32),
            pltpu.SMEM(vent_rate.shape, f32),
            pltpu.VMEM(full.shape, f32),
            pltpu.VMEM((levels, SUBLANES, cols), f32),
            pltpu.VMEM((levels, rows, LANES), f32),
            pltpu.SemaphoreType.DMA((5,)),
            pltpu.SemaphoreType.DMA((3,)),
        ],
        compiler_params=whole_vmem,
        cost_estimate=cost(cells, 10, 2),
    )(
        slot_pick, horiz_diff, class_rates, vent_cells, vent_rate,
        fields, courant_x, courant_y, precip_class,
    )

    west = neighbour(xf, "gx", 1)
    east = neighbour(xb, "gx", -1)
    south = neighbour(yf, "gy", 1)
    north = neighbour(yb, "gy", -1)

    levels_smem = [pltpu.SMEM((levels,), f32)] * 3
    blocks = 4
    pack, mine, at_vents, *later = pl.pallas_call(
        functools.partial(first_kernel, dims, pieces[1:], blocks),
        name="first",
        in_specs=[hbm()] * 8 + [vmem()] * 7,
        out_specs=[hbm(), vmem(), vmem()] + [hbm()] * (len(pieces) - 1),
        out_shape=[shape((levels, SLOTS, rows, cols), f32), rims, shape((vents, 2 * LANES), f32)]
        + [shape((b - a, rows, cols), f32) for a, b in pieces[1:]],
        scratch_shapes=[pltpu.SMEM(slot_pick.shape, i32)]
        + levels_smem
        + [pltpu.SMEM(vent_cells.shape, i32)]
        + [pltpu.VMEM(full.shape, f32)] * 4
        + [
            pltpu.SemaphoreType.DMA((5,)),
            pltpu.SemaphoreType.DMA((blocks, 3)),
            pltpu.SemaphoreType.DMA((blocks, 4)),
            pltpu.SemaphoreType.DMA((len(pieces) - 1,)),
        ],
        compiler_params=whole_vmem,
        cost_estimate=cost(cells, 40, 5),
    )(
        slot_pick, horiz_diff, vert_diff, profile, vent_cells,
        fields, courant_x, courant_y, west, east, south, north, rate, column, edges,
    )

    theirs = send(mine)
    at_vents = neighbour(at_vents, "section", -1)
    for piece in later:
        received.append(send(piece))

    rim, xf, xb, yf, yb, terms = pl.pallas_call(
        functools.partial(rim_kernel, dims),
        name="rim",
        in_specs=[vmem()] * 8,
        out_specs=[vmem()] * 6,
        out_shape=[rims, line, line, side, side, shape((1, vents), f32)],
        compiler_params=params,
        cost_estimate=cost(edge_rows * cols, 20, 5),
    )(profile[None, :], mine, theirs, at_vents, edges, edge_rate, cu0, cv0)
    west = neighbour(xf, "gx", 1)
    east = neighbour(xb, "gx", -1)
    south = neighbour(yf, "gy", 1)
    north = neighbour(yb, "gy", -1)

    def load_window(piece):
        base, (_, end), _ = window_of(piece, levels)
        return shape((end - base, 4, rows, cols), f32)

    window = pl.pallas_call(
        functools.partial(load_kernel, window_of(pieces[0], levels)[0]),
        name="load",
        in_specs=[hbm()],
        out_specs=vmem(),
        out_shape=load_window(pieces[0]),
        scratch_shapes=[pltpu.SemaphoreType.DMA((1,))],
        compiler_params=params,
        cost_estimate=cost(cells, 10, 1),
    )(pack)

    steps = doubling_steps()
    while len(steps) > 2:
        terms = terms + partner(terms, steps.pop(0))

    result = carry = None
    for j, piece in enumerate(pieces):
        low, high = piece
        following = pieces[j + 1] if j + 1 < len(pieces) else None
        base, (_, end), (out0, out1) = window_of(piece, levels)
        outs = out1 - out0
        if steps:
            more = partner(terms, steps.pop(0))
        elif j == 2:
            passed = neighbour(terms, "section", 1)
        operands = [
            horiz_diff, vert_diff, profile, pack, window,
            west, east, south, north, rate, column, rim, received[j],
        ]
        specs = [hbm()] * 4 + [vmem()] * 9
        aliases = {}
        if not following:
            operands += [terms, passed]
            specs += [vmem()] * 2
        if low > 0:
            operands += [carry, result]
            specs += [vmem(), hbm()]
            aliases = {len(operands) - 1: 0}
        out_shape = [full]
        out_specs = [hbm()]
        if following:
            out_shape += [load_window(following), shape((4, rows, cols), f32)]
            out_specs += [vmem(), vmem()]
        else:
            out_shape += [shape((1, vents), f32)]
            out_specs += [vmem()]
        result, *state = pl.pallas_call(
            functools.partial(chunk_kernel, dims, piece, following),
            in_specs=specs,
            out_specs=out_specs,
            out_shape=out_shape,
            scratch_shapes=levels_smem
            + [
                pltpu.VMEM((high - out0, rows, cols), f32),
                pltpu.VMEM((end - base, rows, cols), f32),
                pltpu.VMEM((outs, rows, cols), f32),
                pltpu.SemaphoreType.DMA((3,)),
                pltpu.SemaphoreType.DMA((1,)),
                pltpu.SemaphoreType.DMA((outs,)),
            ],
            input_output_aliases=aliases,
            compiler_params=params,
            cost_estimate=cost((high - low) * rows * cols, 80, 7),
        )(*operands)
        if following:
            window, carry = state
            if j < 2:
                terms = terms + more
        else:
            (terms,) = state
    return (result[None], terms[0])


def solution(mesh):
    return jax.shard_map(
        program,
        mesh=mesh,
        in_specs=(
            P("section", None, None, "gx", "gy"),
            P(),
            P(None, "gx", "gy"),
            P(None, "gx", "gy"),
            P(),
            P(),
            P("gx", "gy"),
            P(),
            P(),
            P(),
            P(),
        ),
        out_specs=(P("section", None, "gx", "gy"), P()),
        check_vma=False,
    )
```

```python
import functools

import jax
import jax.numpy as jnp
from jax import lax
from jax.experimental import pallas as pl
from jax.experimental.pallas import tpu as pltpu
from jax.sharding import PartitionSpec as P

LANES = 128
SUBLANES = 8
SLOTS = 7


def vmem():
    return pl.BlockSpec(memory_space=pltpu.VMEM)


def hbm():
    return pl.BlockSpec(memory_space=pltpu.HBM)


def neighbour(value, axis, by):
    size = lax.axis_size(axis)
    pairs = [(i, i + by) for i in range(size) if 0 <= i + by < size]
    return lax.ppermute(value, axis, pairs)


def doubling_steps():
    wide, deep = lax.axis_size("gx"), lax.axis_size("gy")
    steps = []
    step = 1
    while step < wide * deep:
        steps.append([(i, i ^ step) for i in range(wide * deep)])
        step *= 2
    return steps


def partner(value, pairs):
    return lax.ppermute(value, ("section", "gx", "gy"), pairs)


def inverse(conc):
    return 1.0 / (1.0 + conc * conc)


def wash(conc):
    return conc * conc * inverse(conc)


def slope(conc):
    inv = inverse(conc)
    return 2.0 * conc * inv * inv


def iotas(rows, cols):
    return (
        lax.broadcasted_iota(jnp.int32, (rows, cols), 0),
        lax.broadcasted_iota(jnp.int32, (rows, cols), 1),
    )


def wide(block, cols):
    return jnp.concatenate([block] * (cols // LANES), axis=1)


def lane_to(block, lane, target):
    return pltpu.roll(block, lax.rem(target - lane + 2 * LANES, LANES), 1)


def get_row(ref, r, lanes=slice(None)):
    base = pl.multiple_of((r // SUBLANES) * SUBLANES, SUBLANES)
    block = ref[pl.ds(base, SUBLANES), lanes]
    return pltpu.roll(block, lax.rem(SUBLANES - lax.rem(r, SUBLANES), SUBLANES), 0)[0:1]


def put_row(ref, r, value, lanes=slice(None)):
    base = pl.multiple_of((r // SUBLANES) * SUBLANES, SUBLANES)
    block = ref[pl.ds(base, SUBLANES), lanes]
    sub = lax.broadcasted_iota(jnp.int32, block.shape, 0)
    ref[pl.ds(base, SUBLANES), lanes] = jnp.where(sub == lax.rem(r, SUBLANES), value, block)


class Sides:
    def __init__(self, west, east, south, north):
        self.west, self.east, self.south, self.north = west, east, south, north


def level_coefs(adjoint, z, levels, horiz, vert):
    h = horiz[z]
    k = vert[z]
    if adjoint:
        above = vert[jnp.minimum(z + 1, levels - 1)]
        below = vert[jnp.maximum(z - 1, 0)]
    else:
        above = below = k
    above = jnp.where(z < levels - 1, above, 0.0)
    below = jnp.where(z > 0, below, 0.0)
    return h, k, above, below


def apply_plane(adjoint, z, levels, field, up, down, cu, cv, horiz, vert, sides):
    rows, cols = field.shape
    row, col = iotas(rows, cols)
    h, k, above, below = level_coefs(adjoint, z, levels, horiz, vert)
    if adjoint:
        to_east = (cu + h) * field
        to_north = (cv + h) * field
    else:
        to_east = to_north = h * field
    west = pltpu.roll(field, 1, 0)
    east = pltpu.roll(to_east, rows - 1, 0)
    south = pltpu.roll(field, 1, 1)
    north = pltpu.roll(to_north, cols - 1, 1)
    if sides is not None:
        west = jnp.where(row == 0, get_row(sides.west, z), west)
        east = jnp.where(row == rows - 1, get_row(sides.east, z), east)
        south = jnp.where(col == 0, wide(lane_to(sides.south[...], z, 0), cols), south)
        north = jnp.where(
            col == cols - 1, wide(lane_to(sides.north[...], z, LANES - 1), cols), north
        )
    diag = 1.0 - cu - cv - (4.0 * h + 2.0 * k)
    if adjoint:
        total = diag * field + h * (west + south) + east + north
    else:
        total = diag * field + (cu + h) * west + (cv + h) * south + east + north
    return total + above * up + below * down


def here_of(cells, v, dims):
    _, rows, cols, grid_y = dims
    cell = cells[v]
    if grid_y & (grid_y - 1):
        line = cell // grid_y
    else:
        line = lax.shift_right_logical(cell, jnp.int32(grid_y.bit_length() - 1))
    x = line - lax.axis_index("gx") * rows
    y = cell - line * grid_y - lax.axis_index("gy") * cols
    return x, y, (x >= 0) & (x < rows) & (y >= 0) & (y < cols)


def gather_vents(cells, source, target, dims):
    levels = dims[0]
    _, lane = iotas(SUBLANES, LANES)

    def one(v, carry):
        x, y, here = here_of(cells, v, dims)

        @pl.when(here)
        def _():
            base = pl.multiple_of((y // LANES) * LANES, LANES)
            low = lax.rem(y, LANES)
            top = pl.multiple_of((x // SUBLANES) * SUBLANES, SUBLANES)
            got = jnp.zeros((SUBLANES, LANES), jnp.float32)
            for z in range(levels):
                block = source[z, pl.ds(top, SUBLANES), pl.ds(base, LANES)]
                got = jnp.where(lane == z, lane_to(block, low, z), got)
            got = pltpu.roll(got, lax.rem(SUBLANES - lax.rem(x, SUBLANES), SUBLANES), 0)[0:1]
            put_row(target, v, got, slice(0, LANES))

        return carry

    lax.fori_loop(0, cells.shape[0], one, 0)


def put_columns(target, columns, dims):
    levels, rows = dims[:2]
    half = rows // 2
    at = slice(2 * levels, 2 * levels + half)
    target[at, 0:LANES] = columns[0:half]
    target[at, LANES : 2 * LANES] = columns[half:rows]


def get_columns(source, dims):
    levels, rows = dims[:2]
    at = slice(2 * levels, 2 * levels + rows // 2)
    return jnp.concatenate([source[at, 0:LANES], source[at, LANES : 2 * LANES]], axis=0)


def gather_edges(source, target, dims, blocks=1, ready=lambda b: None):
    levels, rows, cols, _ = dims
    _, lane = iotas(rows, LANES)

    def group(i, columns):
        base = pl.multiple_of(i * SUBLANES, SUBLANES)
        for s in range(SUBLANES):
            z = base + s
            columns = jnp.where(lane == z, lane_to(source[z, :, 0:LANES], 0, z), columns)
            columns = jnp.where(
                lane == z + levels,
                lane_to(source[z, :, cols - LANES : cols], LANES - 1, z + levels),
                columns,
            )
        for top, row in ((0, 0), (levels, rows - 1)):
            lines = [source[base + s, row : row + 1, :] for s in range(SUBLANES)]
            at = pl.multiple_of(top + base, SUBLANES)
            target[pl.ds(at, SUBLANES), :] = jnp.concatenate(lines, axis=0)
        return columns

    zero = jnp.zeros((rows, LANES), jnp.float32)
    columns = zero
    groups = levels // SUBLANES // blocks
    for b in range(blocks):
        ready(b)
        columns = lax.fori_loop(b * groups, (b + 1) * groups, group, columns)
    put_columns(target, columns, dims)


def head_kernel(slot_hbm, fields, out, slot, sems):
    copy = pltpu.make_async_copy(slot_hbm, slot, sems.at[0])
    copy.start()
    copy.wait()
    pick = slot[lax.axis_index("section")]
    copy = pltpu.make_async_copy(fields.at[0, pick, pl.ds(0, out.shape[0])], out, sems.at[1])
    copy.start()
    copy.wait()


def edges_kernel(
    dims,
    slot_hbm,
    horiz_hbm,
    class_hbm,
    cells_hbm,
    vent_hbm,
    fields,
    cu_hbm,
    cv_hbm,
    precip,
    out_xf,
    out_xb,
    out_yf,
    out_yb,
    out_cu0,
    out_cv0,
    out_rate,
    out_column,
    out_edges,
    out_edge_rate,
    out_vents,
    out_vent_rate,
    slot,
    horiz,
    class_rates,
    cells,
    vent_rate,
    field,
    cu,
    cv,
    small_sems,
    sems,
):
    levels, rows, cols, _ = dims
    adj = lax.axis_index("section")
    flag = adj.astype(jnp.float32)
    courants = [
        pltpu.make_async_copy(cv_hbm.at[:, :, pl.ds(0, LANES)], cv, sems.at[0]),
        pltpu.make_async_copy(cu_hbm.at[:, pl.ds(0, SUBLANES), :], cu, sems.at[1]),
    ]
    small = [
        pltpu.make_async_copy(a, b, small_sems.at[i])
        for i, (a, b) in enumerate(
            (
                (slot_hbm, slot),
                (horiz_hbm, horiz),
                (class_hbm, class_rates),
                (cells_hbm, cells),
                (vent_hbm, vent_rate),
            )
        )
    ]
    for copy in small:
        copy.start()
    for copy in courants:
        copy.start()
    for copy in small:
        copy.wait()
    blocks = sems.shape[0] - 2
    size = levels // blocks
    pick = slot[adj]
    copies = [
        pltpu.make_async_copy(
            fields.at[0, pick, pl.ds(b * size, size)],
            field.at[pl.ds(b * size, size)],
            sems.at[2 + b],
        )
        for b in range(blocks)
    ]
    for copy in copies:
        copy.start()

    kinds = precip[...]
    rate = jnp.zeros((rows, cols), jnp.float32)
    for kind in range(class_rates.shape[0]):
        rate = jnp.where(kinds == kind, class_rates[kind], rate)
    out_rate[...] = rate
    out_column[...] = jnp.zeros((rows, cols), jnp.float32)
    out_vents[...] = jnp.zeros(out_vents.shape, jnp.float32)
    out_vent_rate[...] = jnp.zeros(out_vent_rate.shape, jnp.float32)
    _, line_col = iotas(1, cols)

    def one(v, carry):
        x, y, here = here_of(cells, v, dims)

        @pl.when(here)
        def _():
            hit = line_col == y
            line = get_row(out_column, x) + jnp.where(hit, vent_rate[v], 0.0)
            put_row(out_column, x, line)
            found = jnp.sum(jnp.where(hit, get_row(out_rate, x), 0.0), axis=1, keepdims=True)
            found = jnp.broadcast_to(found, (1, LANES))
            put_row(out_vent_rate, v, found)

        return carry

    lax.fori_loop(0, cells.shape[0], one, 0)
    out_edge_rate[0:levels, :] = jnp.broadcast_to(rate[0:1, :], (levels, cols))
    out_edge_rate[levels : 2 * levels, :] = jnp.broadcast_to(rate[rows - 1 : rows, :], (levels, cols))
    _, lane = iotas(rows, LANES)
    put_columns(
        out_edge_rate, jnp.where(lane < levels, rate[:, 0:1], rate[:, cols - 1 : cols]), dims
    )

    for copy in courants:
        copy.wait()

    def group(i, columns):
        base = pl.multiple_of(i * SUBLANES, SUBLANES)
        lines = []
        for s in range(SUBLANES):
            z = base + s
            h = horiz[z]
            block = h + flag * cv[z]
            columns = jnp.where(lane == z, lane_to(block, 0, z), columns)
            lines.append(h + flag * cu[z, 0:1, :])
        out_cu0[pl.ds(base, SUBLANES), :] = jnp.concatenate(lines, axis=0)
        return columns

    zero = jnp.zeros((rows, LANES), jnp.float32)
    out_cv0[...] = lax.fori_loop(0, levels // SUBLANES, group, zero)
    gather_edges(field, out_edges, dims, blocks, lambda b: copies[b].wait())
    gather_vents(cells, field, out_vents, dims)
    columns = get_columns(out_edges, dims)
    out_xf[...] = out_edges[levels : 2 * levels, :]
    out_xb[...] = out_cu0[...] * out_edges[0:levels, :]
    out_yf[...] = pltpu.roll(columns, LANES - levels, 1)
    out_yb[...] = out_cv0[...] * columns


def load_small(pairs, sems):
    copies = [pltpu.make_async_copy(a, b, sems.at[i]) for i, (a, b) in enumerate(pairs)]
    for copy in copies:
        copy.start()
    for copy in copies:
        copy.wait()


def first_kernel(
    dims,
    chunks,
    blocks,
    slot_hbm,
    horiz_hbm,
    vert_hbm,
    profile_hbm,
    cells_hbm,
    fields,
    cu_hbm,
    cv_hbm,
    west,
    east,
    south,
    north,
    rate,
    column,
    vents,
    *rest,
):
    levels, _, _, _ = dims
    out_pack, out_edges, out_vents = rest[:3]
    out_chunks = rest[3 : 3 + len(chunks)]
    slot, horiz, vert, profile, cells = rest[3 + len(chunks) : 8 + len(chunks)]
    field, cu, cv, first, small_sems, in_sems, out_sems, chunk_sems = rest[8 + len(chunks) :]
    adj = lax.axis_index("section")
    size = levels // blocks
    spans = [pl.ds(b * size, size) for b in range(blocks)]
    loads = [
        [
            pltpu.make_async_copy(cu_hbm.at[span], cu.at[span], in_sems.at[b, 0]),
            pltpu.make_async_copy(cv_hbm.at[span], cv.at[span], in_sems.at[b, 1]),
        ]
        for b, span in enumerate(spans)
    ]
    for copy in loads[0]:
        copy.start()
    load_small(
        (
            (slot_hbm, slot),
            (horiz_hbm, horiz),
            (vert_hbm, vert),
            (profile_hbm, profile),
            (cells_hbm, cells),
        ),
        small_sems,
    )
    pick = slot[adj]
    for b, span in enumerate(spans):
        copy = pltpu.make_async_copy(fields.at[0, pick, span], field.at[span], in_sems.at[b, 2])
        copy.start()
        if b:
            for other in loads[b]:
                other.start()
        loads[b].append(copy)
    out_vents[:, 0:LANES] = jnp.zeros(vents.shape, jnp.float32)
    out_vents[:, LANES : 2 * LANES] = vents[...]
    sides = Sides(west, east, south, north)

    def planes(adjoint, low, high):
        def plane(z, carry):
            here = field[z]
            up = field[jnp.minimum(z + 1, levels - 1)]
            down = field[jnp.maximum(z - 1, 0)]
            value = apply_plane(
                adjoint, z, levels, here, up, down, cu[z], cv[z], horiz, vert, sides
            )
            if not adjoint:
                value = value - rate[...] * wash(here) + profile[z] * column[...]
            first[z] = value
            return carry

        lax.fori_loop(low, high, plane, 0)

    stores = []
    for copy in loads[0]:
        copy.wait()
    for b, span in enumerate(spans):
        if b + 1 < blocks:
            for copy in loads[b + 1]:
                copy.wait()
        low = b * size
        high = low + size

        @pl.when(adj == 0)
        def _():
            planes(False, low, high)

        @pl.when(adj == 1)
        def _():
            planes(True, low, high)

        for i, part in enumerate((first, cu, cv, field)):
            store = pltpu.make_async_copy(part.at[span], out_pack.at[span, i], out_sems.at[b, i])
            store.start()
            stores.append(store)
    for i, (low, high) in enumerate(chunks):
        span = pl.ds(low, high - low)
        store = pltpu.make_async_copy(field.at[span], out_chunks[i], chunk_sems.at[i])
        store.start()
        stores.append(store)
    gather_edges(first, out_edges, dims)
    gather_vents(cells, first, out_vents, dims)
    for store in stores:
        store.wait()


def rim_kernel(
    dims,
    profile,
    mine,
    theirs,
    my_vents,
    at_vents,
    edges,
    edge_rate,
    vent_rate,
    cu0,
    cv0,
    out_rim,
    out_xf,
    out_xb,
    out_yf,
    out_yb,
    out_terms,
):
    levels, _, _, _ = dims
    adj = lax.axis_index("section")
    lam = mine[...] - edge_rate[...] * slope(theirs[...]) * edges[...]
    rim = jnp.where(adj == 1, lam, mine[...])
    out_rim[...] = rim
    columns = get_columns(rim, dims)
    out_xf[...] = rim[levels : 2 * levels, :]
    out_xb[...] = cu0[...] * rim[0:levels, :]
    out_yf[...] = pltpu.roll(columns, LANES - levels, 1)
    out_yb[...] = cv0[...] * columns
    vents = out_terms.shape[1]
    lam_two = at_vents[:, LANES : 2 * LANES]
    loss = vent_rate[...] * slope(my_vents[:, 0:LANES]) * lam_two
    both = at_vents[:, 0:LANES] - loss + lam_two
    weights = jnp.concatenate(
        [profile[...], jnp.zeros((1, LANES - levels), jnp.float32)], axis=1
    )
    both = jnp.concatenate([both * weights, jnp.zeros((LANES - vents, LANES), jnp.float32)], axis=0)
    sums = jnp.sum(jnp.transpose(both), axis=0, keepdims=True)[:, 0:vents]
    out_terms[...] = sums


def window_of(piece, levels):
    low, high = piece
    last = high == levels
    base = max(low - 3, 0)
    new0 = max(low - 1, 0)
    out0 = max(low - 2, 0)
    new1 = levels if last else high - 1
    out1 = levels if last else high - 2
    return base, (new0, new1), (out0, out1)


def load_kernel(base, pack, out, sem):
    copy = pltpu.make_async_copy(
        pack.at[pl.ds(base, out.shape[0]), pl.ds(0, 4)], out, sem.at[0]
    )
    copy.start()
    copy.wait()


def chunk_kernel(
    dims,
    piece,
    following,
    horiz_hbm,
    vert_hbm,
    profile_hbm,
    pack,
    window,
    west,
    east,
    south,
    north,
    rate,
    column,
    rim,
    arrived,
    *rest,
):
    levels, rows, cols, _ = dims
    low, high = piece
    has_carry = low > 0
    if not following:
        terms, more_terms = rest[:2]
        rest = rest[2:]
    if has_carry:
        carry_in, _ = rest[:2]
        rest = rest[2:]
    out_hbm = rest[0]
    rest = rest[1:]
    if following:
        next_window, carry_out = rest[:2]
        rest = rest[2:]
    else:
        rest[0][...] = jnp.where(lax.axis_index("section") == 1, more_terms[...], terms[...])
        rest = rest[1:]
    horiz, vert, profile, conc, fresh, result, small_sems, next_sem, out_sems = rest
    adj = lax.axis_index("section")
    base, (new0, new1), (out0, out1) = window_of(piece, levels)
    conc0 = out0
    sides = Sides(west, east, south, north)
    if following:
        start, _, _ = window_of(following, levels)
        ahead = pltpu.make_async_copy(
            pack.at[pl.ds(start, next_window.shape[0]), pl.ds(0, 4)], next_window, next_sem.at[0]
        )
        ahead.start()
    load_small(((horiz_hbm, horiz), (vert_hbm, vert), (profile_hbm, profile)), small_sems)

    def store(z):
        return pltpu.make_async_copy(
            result.at[z - out0], out_hbm.at[z], out_sems.at[z - out0]
        )

    @pl.when(adj == 1)
    def _():
        def move(z, carry):
            conc[low - conc0 + z] = arrived[z]
            return carry

        lax.fori_loop(0, high - low, move, 0)
        if has_carry:
            fresh[0:2] = carry_in[0:2]
            conc[0:2] = carry_in[2:4]

        def new_plane(z, carry):
            i = z - conc0
            j = z - base
            here = conc[i]
            up = conc[jnp.minimum(z + 1, levels - 1) - conc0]
            down = conc[jnp.maximum(z - 1, 0) - conc0]
            value = apply_plane(
                False, z, levels, here, up, down, window[j, 1], window[j, 2], horiz, vert, None
            )
            value = value - rate[...] * wash(here) + profile[z] * column[...]
            value = window[j, 0] - rate[...] * slope(value) * window[j, 3]
            row, col = iotas(rows, cols)
            columns = get_columns(rim, dims)
            value = jnp.where(col == 0, wide(lane_to(columns, z, 0), cols), value)
            value = jnp.where(
                col == cols - 1, wide(lane_to(columns, z + levels, LANES - 1), cols), value
            )
            value = jnp.where(row == 0, get_row(rim, z), value)
            value = jnp.where(row == rows - 1, get_row(rim, levels + z), value)
            fresh[j] = value
            return carry

        lax.fori_loop(new0, new1, new_plane, 0)
        if following:
            carry_out[0:2] = fresh[new1 - 2 - base : new1 - base]
            carry_out[2:4] = conc[high - 2 - conc0 : high - conc0]

        def out_plane(z, carry):
            j = z - base
            here = fresh[j]
            up = fresh[jnp.minimum(z + 1, levels - 1) - base]
            down = fresh[jnp.maximum(z - 1, 0) - base]
            value = apply_plane(
                True, z, levels, here, up, down, window[j, 1], window[j, 2], horiz, vert, sides
            )
            result[z - out0] = value - rate[...] * slope(conc[z - conc0]) * here
            store(z).start()
            return carry

        lax.fori_loop(out0, out1, out_plane, 0)

    @pl.when(adj == 0)
    def _():
        def out_plane(z, carry):
            j = z - base
            here = window[j, 0]
            up = window[jnp.minimum(z + 1, levels - 1) - base, 0]
            down = window[jnp.maximum(z - 1, 0) - base, 0]
            value = apply_plane(
                False, z, levels, here, up, down, window[j, 1], window[j, 2], horiz, vert, sides
            )
            result[z - out0] = value - rate[...] * wash(here) + profile[z] * column[...]
            store(z).start()
            return carry

        lax.fori_loop(out0, out1, out_plane, 0)

    def wait(z, carry):
        store(z).wait()
        return carry

    lax.fori_loop(out0, out1, wait, 0)
    if following:
        ahead.wait()


def cost(cells, ops, arrays):
    return pl.CostEstimate(flops=cells * ops, bytes_accessed=4 * cells * arrays, transcendentals=0)


def cuts(levels):
    sizes = [levels * part // 64 for part in (32, 16, 10, 4)]
    sizes.append(levels - sum(sizes))
    bounds = [0]
    for size in sizes:
        bounds.append(bounds[-1] + size)
    return list(zip(bounds[:-1], bounds[1:]))


def program(
    fields,
    slot_pick,
    courant_x,
    courant_y,
    horiz_diff,
    vert_diff,
    precip_class,
    class_rates,
    vent_cells,
    vent_rate,
    profile,
):
    levels, rows, cols = courant_x.shape
    vents = vent_cells.shape[0]
    grid_y = cols * lax.axis_size("gy")
    dims = (levels, rows, cols, grid_y)
    cells = levels * rows * cols
    edge_rows = 2 * levels + rows // 2
    f32 = jnp.float32
    i32 = jnp.int32
    shape = jax.ShapeDtypeStruct
    full = shape((levels, rows, cols), f32)
    line = shape((levels, cols), f32)
    side = shape((rows, LANES), f32)
    flat = shape((rows, cols), f32)
    rims = shape((edge_rows, cols), f32)
    vent_rows = shape((vents, LANES), f32)
    pieces = cuts(levels)

    whole_vmem = pltpu.CompilerParams(vmem_limit_bytes=58 * 1024 * 1024)
    params = pltpu.CompilerParams(vmem_limit_bytes=34 * 1024 * 1024)
    head_params = pltpu.CompilerParams(vmem_limit_bytes=45 * 1024 * 1024)

    def send(value):
        return neighbour(value, "section", 1)

    low, high = pieces[0]
    start = pl.pallas_call(
        head_kernel,
        name="head",
        in_specs=[hbm()] * 2,
        out_specs=vmem(),
        out_shape=shape((high - low, rows, cols), f32),
        scratch_shapes=[pltpu.SMEM(slot_pick.shape, i32), pltpu.SemaphoreType.DMA((2,))],
        compiler_params=head_params,
        cost_estimate=cost(cells, 1, 1),
    )(slot_pick, fields)
    received = [send(start)]

    (
        xf, xb, yf, yb, cu0, cv0, rate, column, edges, edge_rate, my_vents, vent_rates
    ) = pl.pallas_call(
        functools.partial(edges_kernel, dims),
        name="edges",
        in_specs=[hbm()] * 8 + [vmem()],
        out_specs=[vmem()] * 12,
        out_shape=[line, line, side, side, line, side, flat, flat, rims, rims]
        + [vent_rows] * 2,
        scratch_shapes=[
            pltpu.SMEM(slot_pick.shape, i32),
            pltpu.SMEM(horiz_diff.shape, f32),
            pltpu.SMEM(class_rates.shape, f32),
            pltpu.SMEM(vent_cells.shape, i32),
            pltpu.SMEM(vent_rate.shape, f32),
            pltpu.VMEM(full.shape, f32),
            pltpu.VMEM((levels, SUBLANES, cols), f32),
            pltpu.VMEM((levels, rows, LANES), f32),
            pltpu.SemaphoreType.DMA((5,)),
            pltpu.SemaphoreType.DMA((6,)),
        ],
        compiler_params=whole_vmem,
        cost_estimate=cost(cells, 10, 2),
    )(
        slot_pick, horiz_diff, class_rates, vent_cells, vent_rate,
        fields, courant_x, courant_y, precip_class,
    )

    west = neighbour(xf, "gx", 1)
    east = neighbour(xb, "gx", -1)
    south = neighbour(yf, "gy", 1)
    north = neighbour(yb, "gy", -1)

    levels_smem = [pltpu.SMEM((levels,), f32)] * 3
    blocks = 8
    pack, mine, my_vents, *later = pl.pallas_call(
        functools.partial(first_kernel, dims, pieces[1:], blocks),
        name="first",
        in_specs=[hbm()] * 8 + [vmem()] * 7,
        out_specs=[hbm(), vmem(), vmem()] + [hbm()] * (len(pieces) - 1),
        out_shape=[shape((levels, SLOTS, rows, cols), f32), rims, shape((vents, 2 * LANES), f32)]
        + [shape((b - a, rows, cols), f32) for a, b in pieces[1:]],
        scratch_shapes=[pltpu.SMEM(slot_pick.shape, i32)]
        + levels_smem
        + [pltpu.SMEM(vent_cells.shape, i32)]
        + [pltpu.VMEM(full.shape, f32)] * 4
        + [
            pltpu.SemaphoreType.DMA((5,)),
            pltpu.SemaphoreType.DMA((blocks, 3)),
            pltpu.SemaphoreType.DMA((blocks, 4)),
            pltpu.SemaphoreType.DMA((len(pieces) - 1,)),
        ],
        compiler_params=whole_vmem,
        cost_estimate=cost(cells, 40, 5),
    )(
        slot_pick, horiz_diff, vert_diff, profile, vent_cells,
        fields, courant_x, courant_y, west, east, south, north, rate, column, my_vents,
    )

    theirs = send(mine)
    at_vents = neighbour(my_vents, "section", -1)
    for piece in later:
        received.append(send(piece))

    rim, xf, xb, yf, yb, terms = pl.pallas_call(
        functools.partial(rim_kernel, dims),
        name="rim",
        in_specs=[vmem()] * 10,
        out_specs=[vmem()] * 6,
        out_shape=[rims, line, line, side, side, shape((1, vents), f32)],
        compiler_params=params,
        cost_estimate=cost(edge_rows * cols, 20, 5),
    )(
        profile[None, :], mine, theirs, my_vents, at_vents, edges, edge_rate, vent_rates, cu0, cv0
    )
    west = neighbour(xf, "gx", 1)
    east = neighbour(xb, "gx", -1)
    south = neighbour(yf, "gy", 1)
    north = neighbour(yb, "gy", -1)

    def load_window(piece):
        base, (_, end), _ = window_of(piece, levels)
        return shape((end - base, 4, rows, cols), f32)

    window = pl.pallas_call(
        functools.partial(load_kernel, window_of(pieces[0], levels)[0]),
        name="load",
        in_specs=[hbm()],
        out_specs=vmem(),
        out_shape=load_window(pieces[0]),
        scratch_shapes=[pltpu.SemaphoreType.DMA((1,))],
        compiler_params=params,
        cost_estimate=cost(cells, 10, 1),
    )(pack)

    steps = doubling_steps()
    while len(steps) > 3:
        terms = terms + partner(terms, steps.pop(0))

    result = carry = None
    for j, piece in enumerate(pieces):
        low, high = piece
        following = pieces[j + 1] if j + 1 < len(pieces) else None
        base, (_, end), (out0, out1) = window_of(piece, levels)
        outs = out1 - out0
        if steps:
            more = partner(terms, steps.pop(0))
        elif j == 3:
            passed = neighbour(terms, "section", 1)
        operands = [
            horiz_diff, vert_diff, profile, pack, window,
            west, east, south, north, rate, column, rim, received[j],
        ]
        specs = [hbm()] * 4 + [vmem()] * 9
        aliases = {}
        if not following:
            operands += [terms, passed]
            specs += [vmem()] * 2
        if low > 0:
            operands += [carry, result]
            specs += [vmem(), hbm()]
            aliases = {len(operands) - 1: 0}
        out_shape = [full]
        out_specs = [hbm()]
        if following:
            out_shape += [load_window(following), shape((4, rows, cols), f32)]
            out_specs += [vmem(), vmem()]
        else:
            out_shape += [shape((1, vents), f32)]
            out_specs += [vmem()]
        result, *state = pl.pallas_call(
            functools.partial(chunk_kernel, dims, piece, following),
            in_specs=specs,
            out_specs=out_specs,
            out_shape=out_shape,
            scratch_shapes=levels_smem
            + [
                pltpu.VMEM((high - out0, rows, cols), f32),
                pltpu.VMEM((end - base, rows, cols), f32),
                pltpu.VMEM((outs, rows, cols), f32),
                pltpu.SemaphoreType.DMA((3,)),
                pltpu.SemaphoreType.DMA((1,)),
                pltpu.SemaphoreType.DMA((outs,)),
            ],
            input_output_aliases=aliases,
            compiler_params=params,
            cost_estimate=cost((high - low) * rows * cols, 80, 7),
        )(*operands)
        if following:
            window, carry = state
            if j < 3:
                terms = terms + more
        else:
            (terms,) = state
    return (result[None], terms[0])


def solution(mesh):
    return jax.shard_map(
        program,
        mesh=mesh,
        in_specs=(
            P("section", None, None, "gx", "gy"),
            P(),
            P(None, "gx", "gy"),
            P(None, "gx", "gy"),
            P(),
            P(),
            P("gx", "gy"),
            P(),
            P(),
            P(),
            P(),
        ),
        out_specs=(P("section", None, "gx", "gy"), P()),
        check_vma=False,
    )
```
